768 devices in a mesh: dp: 12 (over x, z_hi), tensor: 64 (over y, z_lo, core).
Axes of the slice: x: 4, y: 8, z: 12 (z_hi: 3, z_lo: 4; z = z_hi * 4 + z_lo), core: 2. Of those that a mesh axis runs over, the one named last changes fastest.
Arguments:
- queries: bfloat16 [4608, 8192], P('dp', 'tensor'), may hold values from -180 to 180
- keys: bfloat16 [4608, 1024], P('dp'), may hold values from -4.5 to 4.5
- values: bfloat16 [4608, 1024], P('dp'), may hold values from -6 to 6
- grad_out: bfloat16 [4608, 8192], P('dp', 'tensor'), may hold values from -3 to 3
- weight: float32 [8256, 8192], P('dp', 'tensor'), as said below
- first_code: bfloat16 [8256, 8192], P('dp', 'tensor'), may hold values from -1 to 1, as said below
- first_rows: float32 [8256], P('dp'), may hold values from 0.2 to 5
- first_cols: float32 [8192], P('tensor'), may hold values from 0.2 to 5
- second_code: bfloat16 [8256, 8192], P('dp', 'tensor'), may hold values from 0 to 1, as said below
- second_rows: float32 [8256], P('dp'), may hold values from 0.5 to 20
- second_cols: float32 [8192], P('tensor'), may hold values from 0.5 to 20
Outputs:
- grad_queries: bfloat16 [4608, 8192], P('dp', 'tensor')
- new_weight: float32 [8256, 8192], P('dp', 'tensor')
- next_first_code: bfloat16 [8256, 8192], P('dp', 'tensor')
- next_first_rows: float32 [8256], P('dp')
- next_first_cols: float32 [8192], P('tensor')
- next_second_code: bfloat16 [8256, 8192], P('dp', 'tensor')
- next_second_rows: float32 [8256], P('dp')
- next_second_cols: float32 [8192], P('tensor')
The draws below stay inside these ranges and needn't reach their ends.
Inputs may be any that keep to these rules, and one draw needn't show every extreme that they name: `weight`: rows 8192 onward are zero. `first_code`: rows 8192 onward are zero. `second_code`: rows 8192 onward are zero; all other entries are 0.05 or more.
All inputs are finite; a program needn't handle non-finite values.
Results may differ from the reference program's by a relative error of at most 0.023.
Values may be sent and summed in bfloat16 or wider, within the bound.
No kernel may reach another device: no remote copies, remote signals or barrier semaphores. Data moves between devices by JAX's collectives and lax.ppermute only.
A program may use at most 64 MiB of HBM per device.

```python
import math
import jax
import jax.numpy as jnp
from jax import lax

D = 8192
H = 64
KVH = 8
HD = 128
SEQ = 384
TOK = 4608
CPAD = 8256


def paired_draw(key):
    count = TOK // SEQ
    queries = jnp.clip(jax.random.normal(jax.random.fold_in(key, 101), (count, SEQ, H * HD), jnp.float32), -4.5, 4.5)
    keys = jnp.clip(jax.random.normal(jax.random.fold_in(key, 102), (count, SEQ, KVH * HD), jnp.float32), -4.5, 4.5)
    return (queries.reshape(TOK, H * HD), keys.reshape(TOK, KVH * HD))


def draw_queries(key, part):
    return paired_draw(key)[0].astype(jnp.bfloat16)


def draw_keys(key, part):
    return paired_draw(key)[1].astype(jnp.bfloat16)


def real_rows():
    return jnp.arange(CPAD)[:, None] < D


def draw_weight(key, part):
    filled = jax.random.normal(key, (CPAD, H * HD), jnp.float32) * (H * HD) ** (-0.5)
    return jnp.where(real_rows(), filled, 0.0)


def draw_first_code(key, part):
    filled = jax.random.uniform(key, (CPAD, H * HD), jnp.float32, -1.0, 1.0)
    return jnp.where(real_rows(), filled, 0.0).astype(jnp.bfloat16)


def draw_second_code(key, part):
    filled = jax.random.uniform(key, (CPAD, H * HD), jnp.float32, 0.05, 1.0)
    return jnp.where(real_rows(), filled, 0.0).astype(jnp.bfloat16)


def levels(rng, dims, shards, smallest, largest):
    def one(position, parts):
        draws = jax.random.uniform(jax.random.fold_in(jax.random.fold_in(rng, 6), position), (parts,), jnp.float32, smallest / len(shards), largest / len(shards))
        return jnp.repeat(jnp.exp(draws), dims[position] // parts).reshape((-1,) + (1,) * (len(dims) - position - 1))

    loudness = one(*shards[0])
    for cut in shards[1:]:
        loudness = loudness * one(*cut)
    return loudness


def scatter_about(key, dims, spread, most, split=(), dtype=jnp.bfloat16):
    level = levels(key, dims, split, -0.22, 0.18) if split else 1.0
    array = jax.random.normal(key, dims, jnp.float32) * spread * level
    return jnp.minimum(jnp.maximum(array, -most), most).astype(dtype)


def setup_inputs(seed: int = 0) -> dict:
    streams_of = jax.random.split(jax.random.key(seed), 12)
    return {
        "queries": draw_queries(jax.random.fold_in(streams_of[11], 71), 0),
        "keys": draw_keys(jax.random.fold_in(streams_of[11], 71), 0),
        "values": scatter_about(streams_of[2], (TOK, KVH * HD), 1.0, 6.0, ((0, 12),)),
        "grad_out": scatter_about(streams_of[3], (TOK, D), 0.5, 3.0, ((0, 12), (1, 64))),
        "weight": draw_weight(jax.random.fold_in(streams_of[11], 71), 0),
        "first_code": draw_first_code(jax.random.fold_in(streams_of[11], 71), 0),
        "first_rows": jnp.clip(jnp.exp(math.log(5.0) - 3.218876 * jax.random.uniform(streams_of[6], (CPAD,), jnp.float32) ** levels(streams_of[6], (CPAD,), ((0, 12),), -0.2, 0.2)), 0.2, 5.0),
        "first_cols": jnp.clip(jnp.exp(math.log(5.0) - 3.218876 * jax.random.uniform(streams_of[7], (H * HD,), jnp.float32) ** levels(streams_of[7], (H * HD,), ((0, 64),), -0.2, 0.2)), 0.2, 5.0),
        "second_code": draw_second_code(jax.random.fold_in(streams_of[11], 71), 0),
        "second_rows": jnp.clip(jnp.exp(math.log(20.0) - 3.6888795 * jax.random.uniform(streams_of[9], (CPAD,), jnp.float32) ** levels(streams_of[9], (CPAD,), ((0, 12),), -0.2, 0.2)), 0.5, 20.0),
        "second_cols": jnp.clip(jnp.exp(math.log(20.0) - 3.6888795 * jax.random.uniform(streams_of[10], (H * HD,), jnp.float32) ** levels(streams_of[10], (H * HD,), ((0, 64),), -0.2, 0.2)), 0.5, 20.0),
    }


beta_first = 0.9
beta_second = 0.95
learning = 0.01
decay_rate = 0.1
adam_eps = 1e-08
code_eps = 1e-06
correct_first = 1.0 - 0.9 ** 10
correct_second = 1.0 - 0.95 ** 10

def reference(queries, keys, values, grad_out, weight, first_code, first_rows, first_cols, second_code, second_rows, second_cols):
    count = queries.shape[0] // SEQ
    group = H // KVH
    factor = HD ** (-0.5)
    weight_half = weight.astype(jnp.bfloat16)
    grad_att = jnp.dot(grad_out, weight_half[:D], preferred_element_type=jnp.float32)
    grad_half = grad_att.astype(jnp.bfloat16)
    future = jnp.arange(SEQ)[None, :] > jnp.arange(SEQ)[:, None]

    def per_sequence(inputs):
        query_block, key_block, value_block, grad_block = inputs
        query_heads = query_block.reshape(SEQ, H, HD).astype(jnp.float32)
        key_heads = jnp.repeat(key_block.reshape(SEQ, KVH, HD), group, axis=1).astype(jnp.float32)
        value_heads = jnp.repeat(value_block.reshape(SEQ, KVH, HD), group, axis=1).astype(jnp.float32)
        scores = jnp.einsum('qhd,khd->hqk', query_heads, key_heads) * factor
        scores = jnp.where(future[None], -1e+30, scores)
        highest = lax.optimization_barrier(jnp.max(scores, axis=-1, keepdims=True))
        exponent = jnp.exp(scores - highest)
        probabilities = exponent / lax.optimization_barrier(jnp.sum(exponent, axis=-1, keepdims=True))
        weights_half = probabilities.astype(jnp.bfloat16)
        attended = jnp.einsum('hqk,khd->qhd', weights_half.astype(jnp.float32), value_heads).astype(jnp.bfloat16)
        grad_heads = grad_block.reshape(SEQ, H, HD).astype(jnp.float32)
        grad_probs = jnp.einsum('qhd,khd->hqk', grad_heads, value_heads)
        row_dot = lax.optimization_barrier(jnp.sum(grad_heads * attended.astype(jnp.float32), axis=-1))
        grad_scores = (probabilities * (grad_probs - row_dot.T[:, :, None])).astype(jnp.bfloat16)
        grad_query = (jnp.einsum('hqk,khd->qhd', grad_scores.astype(jnp.float32), key_heads) * factor).astype(jnp.bfloat16)
        return (grad_query.reshape(SEQ, H * HD), attended.reshape(SEQ, H * HD))
    grad_queries, attended = lax.map(per_sequence, (queries.reshape(count, SEQ, H * HD), keys.reshape(count, SEQ, KVH * HD), values.reshape(count, SEQ, KVH * HD), grad_half.reshape(count, SEQ, H * HD)))

    def accumulate(total, inputs):
        grad_block, att_block = inputs
        term = jnp.dot(grad_block.T, att_block, preferred_element_type=jnp.float32)
        return (total + lax.optimization_barrier(term.astype(jnp.bfloat16)).astype(jnp.float32), 0)
    weight_grad, unused = lax.scan(accumulate, jnp.zeros((D, H * HD), jnp.float32), (grad_out.reshape(count, SEQ, D), attended))
    weight_grad = jnp.pad(weight_grad, ((0, CPAD - D), (0, 0)))
    first = first_code.astype(jnp.float32) * jnp.minimum(first_rows[:, None], first_cols[None, :])
    second = second_code.astype(jnp.float32) * jnp.minimum(second_rows[:, None], second_cols[None, :])
    first_new = beta_first * first + (1.0 - beta_first) * weight_grad
    second_new = beta_second * second + (1.0 - beta_second) * weight_grad * weight_grad
    step_size = first_new / correct_first / (jnp.sqrt(second_new / correct_second) + adam_eps)
    new_weight = weight - learning * (step_size + decay_rate * weight)
    first_abs = jnp.abs(first_new)
    second_abs = jnp.abs(second_new)
    next_first_rows = lax.optimization_barrier(jnp.max(first_abs, axis=1))
    next_first_cols = lax.optimization_barrier(jnp.max(first_abs, axis=0))
    next_second_rows = lax.optimization_barrier(jnp.max(second_abs, axis=1))
    next_second_cols = lax.optimization_barrier(jnp.max(second_abs, axis=0))
    next_first_code = (first_new / (jnp.minimum(next_first_rows[:, None], next_first_cols[None, :]) + code_eps)).astype(jnp.bfloat16)
    next_second_code = (second_new / (jnp.minimum(next_second_rows[:, None], next_second_cols[None, :]) + code_eps)).astype(jnp.bfloat16)
    return (grad_queries.reshape(count * SEQ, H * HD), new_weight, next_first_code, next_first_rows, next_first_cols, next_second_code, next_second_rows, next_second_cols)
```

```python
import jax
import jax.numpy as jnp
from jax import lax
from jax.sharding import Mesh
from jax.sharding import PartitionSpec as P

H = 64
KVH = 8
HD = 128
DP = ("x", "zh")
TENSOR = ("y", "zl", "c")


beta_first = 0.9
beta_second = 0.95
learning = 0.01
decay_rate = 0.1
adam_eps = 1e-08
code_eps = 1e-06
correct_first = 1.0 - 0.9**10
correct_second = 1.0 - 0.95**10
half = jnp.bfloat16
full = jnp.float32


def shifted(block, axis, distance):
    size = lax.axis_size(axis)
    return lax.ppermute(block, axis, [(k, (k + distance) % size) for k in range(size)])


def gathered(block, axis):
    size = lax.axis_size(axis)
    me = lax.axis_index(axis)
    parts = [block] + [shifted(block, axis, d) for d in range(1, size)]
    stack = jnp.stack(parts)
    order = (me - jnp.arange(size)) % size
    return jnp.take(stack, order, axis=0)


def exchanged(blocks, axis):
    size = lax.axis_size(axis)
    me = lax.axis_index(axis)
    pick = lambda k: lax.dynamic_index_in_dim(blocks, k % size, 0, keepdims=False)
    return [pick(me)] + [shifted(pick(me + d), axis, d) for d in range(1, size)]


def summed(parts):
    total = parts[0].astype(full)
    for part in parts[1:]:
        total = total + part.astype(full)
    return total


def all_to_all(blocks, axes):
    return lax.all_to_all(blocks, axes, split_axis=0, concat_axis=0, tiled=True)


def attend(queries, key_sel, value_sel):
    length = queries.shape[0]
    scores = jnp.dot(queries, key_sel.T, preferred_element_type=full) * HD ** (-0.5)
    future = lax.broadcasted_iota(jnp.int32, (length, length), 1) > lax.broadcasted_iota(
        jnp.int32, (length, length), 0
    )
    scores = jnp.where(future, -1e30, scores)
    highest = jnp.max(scores, axis=-1, keepdims=True)
    exponent = jnp.exp(scores - highest)
    probabilities = exponent / jnp.sum(exponent, axis=-1, keepdims=True)
    attended = jnp.dot(probabilities.astype(half), value_sel, preferred_element_type=full)
    return probabilities, attended.astype(half)


def attend_back(probabilities, attended, grad_half, key_sel, value_sel):
    grad_probs = jnp.dot(grad_half, value_sel.T, preferred_element_type=full)
    row_dot = jnp.sum(grad_half.astype(full) * attended.astype(full), axis=-1, keepdims=True)
    grad_scores = (probabilities * (grad_probs - row_dot)).astype(half)
    return (jnp.dot(grad_scores, key_sel, preferred_element_type=full) * HD ** (-0.5)).astype(half)


def per_device(
    queries,
    keys,
    values,
    grad_out,
    weight,
    first_code,
    first_rows,
    first_cols,
    second_code,
    second_rows,
    second_cols,
):
    dp_count = lax.axis_size(DP)
    tensor_count = lax.axis_size(TENSOR)
    ys, zls, cs = lax.axis_size("y"), lax.axis_size("zl"), lax.axis_size("c")
    xs, zhs = lax.axis_size("x"), lax.axis_size("zh")
    seq = queries.shape[0]
    rows = weight.shape[0]
    few = seq // tensor_count
    quarter = seq // zls
    core = lax.axis_index("c")
    tensor_index = lax.axis_index(TENSOR)
    kv_start = tensor_index // (H // KVH) * HD

    units = grad_out.reshape(zls, ys, cs, few, HD).transpose(1, 0, 2, 3, 4)
    units = all_to_all(units.reshape(tensor_count, few, HD), TENSOR)
    wide = units.transpose(1, 0, 2).reshape(few, tensor_count * HD)
    wide = jnp.pad(wide, ((0, 0), (0, dp_count * rows - wide.shape[1])))
    mine = all_to_all(wide.reshape(few, dp_count, rows).transpose(1, 0, 2), DP)
    mine = mine.reshape(1, dp_count * few, rows)
    near = all_to_all(jnp.broadcast_to(mine, (ys, *mine.shape[1:])), "y")
    near = near.reshape(ys * dp_count * few, rows)
    far = shifted(near, "c", 1)

    key_sel = lax.dynamic_slice_in_dim(keys, kv_start, HD, 1)
    value_sel = lax.dynamic_slice_in_dim(values, kv_start, HD, 1)
    probabilities, attended = attend(queries, key_sel, value_sel)
    got = gathered_cols(attended.reshape(zls, quarter, HD), "zl")
    att = gathered(gathered(got, "zh"), "x").reshape(dp_count, ys, cs, few, zls * HD)
    att = att.transpose(2, 1, 0, 3, 4).reshape(cs, ys * dp_count * few, zls * HD)

    weight_half = weight.astype(half)
    weight_cols = gathered(weight_half, "zl").transpose(1, 0, 2).reshape(rows, zls * HD)

    dims = (((0,), (0,)), ((), ()))
    partial = lax.dot_general(near, att[core], dims, preferred_element_type=full)
    partial = partial + lax.dot_general(far, att[1 - core], dims, preferred_element_type=full)
    partial = partial.astype(half).reshape(rows, zls, HD).transpose(1, 0, 2)
    weight_grad = jnp.sum(all_to_all(partial, "zl").astype(full), axis=0)

    first = first_code.astype(full) * jnp.minimum(first_rows[:, None], first_cols[None, :])
    second = second_code.astype(full) * jnp.minimum(second_rows[:, None], second_cols[None, :])
    first_new = beta_first * first + (1.0 - beta_first) * weight_grad
    second_new = beta_second * second + (1.0 - beta_second) * weight_grad * weight_grad
    step_size = first_new / correct_first / (jnp.sqrt(second_new / correct_second) + adam_eps)
    new_weight = weight - learning * (step_size + decay_rate * weight)
    first_abs = jnp.abs(first_new)
    second_abs = jnp.abs(second_new)
    rows_max = jnp.stack([jnp.max(first_abs, axis=1), jnp.max(second_abs, axis=1)])
    cols_max = jnp.stack([jnp.max(first_abs, axis=0), jnp.max(second_abs, axis=0)])
    rows_max = jnp.max(lax.all_gather(rows_max, "c"), axis=0)
    rows_max = jnp.max(
        all_to_all(jnp.broadcast_to(rows_max[None], (ys * zls, *rows_max.shape)), ("y", "zl")), axis=0
    )
    for axis in ("zh", "x"):
        for_all = [cols_max] + [shifted(cols_max, axis, d) for d in range(1, lax.axis_size(axis))]
        for other in for_all[1:]:
            cols_max = jnp.maximum(cols_max, other)
    next_first_code = (
        first_new / (jnp.minimum(rows_max[0][:, None], cols_max[0][None, :]) + code_eps)
    ).astype(half)
    next_second_code = (
        second_new / (jnp.minimum(rows_max[1][:, None], cols_max[1][None, :]) + code_eps)
    ).astype(half)

    both = jnp.concatenate([near, far], axis=0)
    grad_part = jnp.dot(both, weight_cols, preferred_element_type=full).astype(half)
    grad_part = grad_part.reshape(cs, ys, dp_count, few, zls * HD)
    grad_part = jnp.where(core == 0, grad_part, grad_part[::-1])
    grad_part = grad_part.transpose(2, 1, 0, 3, 4).reshape(xs, zhs * quarter, zls * HD)
    grad_sum = summed(exchanged(grad_part, "x")).astype(half)
    grad_sum = summed(exchanged(grad_sum.reshape(zhs, quarter, zls * HD), "zh")).astype(half)
    grad_half = regrouped_rows(grad_sum.reshape(quarter, zls, HD).transpose(1, 0, 2), "zl")
    grad_queries = attend_back(probabilities, attended, grad_half, key_sel, value_sel)
    return (
        grad_queries,
        new_weight,
        next_first_code,
        rows_max[0],
        cols_max[0],
        next_second_code,
        rows_max[1],
        cols_max[1],
    )


def in_order(parts, axis):
    size = lax.axis_size(axis)
    me = lax.axis_index(axis)
    return jnp.take(jnp.stack(parts), (me - jnp.arange(size)) % size, axis=0)


def gathered_cols(blocks, axis):
    parts = in_order(exchanged(blocks, axis), axis)
    return parts.transpose(1, 0, 2).reshape(blocks.shape[1], -1)


def regrouped_rows(blocks, axis):
    parts = in_order(exchanged(blocks, axis), axis)
    return parts.reshape(-1, blocks.shape[2])


def solution(mesh):
    finer = Mesh(mesh.devices.reshape(4, 3, 8, 4, 2), (*DP, *TENSOR))
    placed = (
        P(DP, TENSOR),
        P(DP, None),
        P(DP, None),
        P(DP, TENSOR),
        P(DP, TENSOR),
        P(DP, TENSOR),
        P(DP),
        P(TENSOR),
        P(DP, TENSOR),
        P(DP),
        P(TENSOR),
    )
    return jax.shard_map(
        per_device,
        mesh=finer,
        in_specs=placed,
        out_specs=(
            P(DP, TENSOR),
            P(DP, TENSOR),
            P(DP, TENSOR),
            P(DP),
            P(TENSOR),
            P(DP, TENSOR),
            P(DP),
            P(TENSOR),
        ),
        check_vma=False,
    )
```

```python
import jax
import jax.numpy as jnp
from jax import lax
from jax.experimental import pallas as pl
from jax.experimental.pallas import tpu as pltpu
from jax.sharding import Mesh
from jax.sharding import PartitionSpec as P

H = 64
KVH = 8
HD = 128
DP = ("x", "zh")
TENSOR = ("y", "zl", "c")
ZHS = 3


beta_first = 0.9
beta_second = 0.95
learning = 0.01
decay_rate = 0.1
adam_eps = 1e-08
code_eps = 1e-06
correct_first = 1.0 - 0.9**10
correct_second = 1.0 - 0.95**10
half = jnp.bfloat16
full = jnp.float32


def shifted(block, axis, distance):
    size = lax.axis_size(axis)
    return lax.ppermute(block, axis, [(k, (k + distance) % size) for k in range(size)])


def gathered(block, axis):
    size = lax.axis_size(axis)
    return [block] + [shifted(block, axis, d) for d in range(1, size)]


def exchanged(blocks, axis):
    size = lax.axis_size(axis)
    return [blocks[0]] + [shifted(blocks[d], axis, d) for d in range(1, size)]


def swapped(block, axis, bit):
    size = lax.axis_size(axis)
    return lax.ppermute(block, axis, [(k, k ^ bit) for k in range(size)])


def back(blocks):
    return [blocks[-d % len(blocks)] for d in range(len(blocks))]


def summed(parts):
    total = parts[0].astype(full)
    for part in parts[1:]:
        total = total + part.astype(full)
    return total


def all_to_all(blocks, axes):
    return lax.all_to_all(blocks, axes, split_axis=0, concat_axis=0, tiled=True)


def attend(queries, key_sel, value_sel, first, per_head):
    shape = (queries.shape[0], key_sel.shape[0])
    scores = jnp.dot(queries, key_sel.T, preferred_element_type=full) * HD ** (-0.5)
    place = lax.broadcasted_iota(jnp.int32, (shape[0] // per_head, per_head, shape[1]), 1).reshape(shape)
    future = lax.broadcasted_iota(jnp.int32, shape, 1) > place + first
    scores = jnp.where(future, -1e30, scores)
    highest = jnp.max(scores, axis=-1, keepdims=True)
    exponent = jnp.exp(scores - highest)
    probabilities = exponent / jnp.sum(exponent, axis=-1, keepdims=True)
    attended = jnp.dot(probabilities.astype(half), value_sel, preferred_element_type=full)
    return probabilities, attended.astype(half)


def attend_back(probabilities, attended, grad_half, key_sel, value_sel):
    grad_probs = jnp.dot(grad_half, value_sel.T, preferred_element_type=full)
    row_dot = jnp.sum(grad_half.astype(full) * attended.astype(full), axis=-1, keepdims=True)
    grad_scores = (probabilities * (grad_probs - row_dot)).astype(half)
    return (jnp.dot(grad_scores, key_sel, preferred_element_type=full) * HD ** (-0.5)).astype(half)


def grad_kernel(sizes, at_ref, near_ref, far_ref, *refs):
    att_refs, (out_ref, cot_ref) = refs[:-2], refs[-2:]
    xs, zhs, ys, cs, few = sizes
    per_seq, rows = ys * cs * few, cot_ref.shape[1]
    count = xs * zhs * per_seq
    x, zh, zl, core = at_ref[0], at_ref[1], at_ref[2], at_ref[3]
    column = lax.broadcasted_iota(jnp.int32, (1, count // cs), 1)
    y = divided(column, xs * zhs * few)
    left = column - y * (xs * zhs * few)
    seq = divided(left, few)
    token = left - seq * few
    seq_x = divided(seq, zhs)
    back_x = x - seq_x
    back_x = jnp.where(back_x < 0, back_x + xs, back_x)
    back_zh = zh - (seq - seq_x * zhs)
    back_zh = jnp.where(back_zh < 0, back_zh + zhs, back_zh)
    place = (back_x * zhs + back_zh) * per_seq + y * (cs * few) + token
    row = lax.broadcasted_iota(jnp.int32, (count, count // cs), 0)
    ordered = None
    for side, part in enumerate((near_ref, far_ref)):
        held = core if side == 0 else 1 - core
        move = (row == place + held * few).astype(half)
        term = jnp.dot(move, part[...], preferred_element_type=full)
        ordered = term if ordered is None else ordered + term
    ordered = ordered[:, :rows].astype(half)
    cot_ref[...] = ordered
    heads = out_ref.shape[0]
    blocks = []
    for ref in att_refs:
        for k in range(zhs):
            start = k * heads * per_seq
            blocks.append(
                jnp.concatenate([ref[start + h * per_seq : start + (h + 1) * per_seq, :] for h in range(heads)], axis=1)
            )
    att = jnp.concatenate(blocks, axis=0)
    total = lax.dot_general(ordered, att, (((0,), (0,)), ((), ())), preferred_element_type=full)
    for h in range(heads):
        out_ref[zl ^ h] = total[:, h * HD : (h + 1) * HD].astype(half)


def divided(value, by):
    return lax.shift_right_logical(value * (65536 // by + 1), 16)


def cot_kernel(cot_ref, two_ref, far_ref, *part_refs):
    weight = jnp.concatenate([two_ref[0], far_ref[0], two_ref[1], far_ref[1]], axis=1)
    heads = weight.shape[1] // HD
    count = cot_ref.shape[0] // len(part_refs)
    per_seq = part_refs[0].shape[0] // (heads * ZHS)
    for k, part_ref in enumerate(part_refs):
        part = jnp.dot(cot_ref[k * count : (k + 1) * count, :], weight, preferred_element_type=full).astype(half)
        for z in range(ZHS):
            for h in range(heads):
                start = (z * heads + h) * per_seq
                part_ref[start : start + per_seq, :] = part[z * per_seq : (z + 1) * per_seq, h * HD : (h + 1) * HD]


def step(
    queries,
    keys,
    values,
    grad_out,
    weight,
    first_code,
    first_rows,
    first_cols,
    second_code,
    second_rows,
    second_cols,
):
    dp_count = lax.axis_size(DP)
    tensor_count = lax.axis_size(TENSOR)
    ys, zls, cs = lax.axis_size("y"), lax.axis_size("zl"), lax.axis_size("c")
    xs, zhs = lax.axis_size("x"), lax.axis_size("zh")
    seq = queries.shape[0]
    rows = weight.shape[0]
    few = seq // tensor_count
    quarter = seq // zls
    tensor_index = lax.axis_index(TENSOR)
    kv_start = tensor_index // (H // KVH) * HD

    zl_at = lax.axis_index("zl")
    zl_order = zl_at ^ jnp.array([0, 2, 1, 3])
    quarters = jnp.take(queries.reshape(zls, quarter, HD), zl_order, axis=0, mode="clip")
    came = swapped(jnp.stack([quarters[1], quarters[3]]), "zl", 2)
    last = swapped(jnp.stack([quarters[2], came[1]]), "zl", 1)
    stacked = jnp.concatenate([quarters[0], last[0], came[0], last[1]], axis=0)

    units = all_to_all(grad_out.reshape(tensor_count, few, HD), ("zl", "y", "c"))
    units = units.reshape(zls, ys, cs, few, HD).transpose(3, 1, 0, 2, 4)
    wide = units.reshape(few, tensor_count * HD)
    wide = jnp.pad(wide, ((0, 0), (0, dp_count * rows - wide.shape[1])))
    lanes = -(-rows // HD) * HD
    wide = jnp.pad(wide.reshape(few, dp_count, rows).transpose(1, 0, 2), ((0, 0), (0, 0), (0, lanes - rows)))
    mine = all_to_all(wide, DP)
    mine = mine.reshape(1, dp_count * few, lanes)
    near = all_to_all(jnp.broadcast_to(mine, (ys, *mine.shape[1:])), "y")
    near = near.reshape(ys * dp_count * few, lanes)
    far = shifted(near, "c", 1)

    key_sel = lax.dynamic_slice_in_dim(keys, kv_start, HD, 1)
    value_sel = lax.dynamic_slice_in_dim(values, kv_start, HD, 1)
    probabilities, attended = attend(stacked, key_sel, value_sel, zl_at * quarter, quarter)
    attended, weight_half = lax.optimization_barrier((attended, weight.astype(half)))
    att = gathered(jnp.concatenate(gathered(attended, "zh"), axis=0), "x")

    weight_two = jnp.stack([weight_half, swapped(weight_half, "zl", 2)])
    weight_far = swapped(weight_two, "zl", 1)

    at = jnp.stack([lax.axis_index(axis) for axis in ("x", "zh", "zl", "c")]).astype(jnp.int32)
    vmem = pl.BlockSpec(memory_space=pltpu.VMEM)
    partial, cot = pl.pallas_call(
        lambda *refs: grad_kernel((xs, zhs, ys, cs, few), *refs),
        out_shape=(jax.ShapeDtypeStruct((zls, rows, HD), half), jax.ShapeDtypeStruct((dp_count * quarter, rows), half)),
        in_specs=[pl.BlockSpec(memory_space=pltpu.SMEM)] + [vmem] * (2 + xs),
        out_specs=(vmem, vmem),
        cost_estimate=pl.CostEstimate(flops=2500000000, bytes_accessed=6000000, transcendentals=0),
    )(at, near, far, *att)
    weight_grad = jnp.sum(all_to_all(partial, "zl").astype(full), axis=0)

    first = first_code.astype(full) * jnp.minimum(first_rows[:, None], first_cols[None, :])
    second = second_code.astype(full) * jnp.minimum(second_rows[:, None], second_cols[None, :])
    first_new = beta_first * first + (1.0 - beta_first) * weight_grad
    second_new = beta_second * second + (1.0 - beta_second) * weight_grad * weight_grad
    step_size = first_new / correct_first / (jnp.sqrt(second_new / correct_second) + adam_eps)
    new_weight = weight - learning * (step_size + decay_rate * weight)
    first_abs = jnp.abs(first_new)
    second_abs = jnp.abs(second_new)
    rows_max = jnp.stack([jnp.max(first_abs, axis=1), jnp.max(second_abs, axis=1)])
    cols_max = jnp.stack([jnp.max(first_abs, axis=0), jnp.max(second_abs, axis=0)])
    rows_max = jnp.max(lax.all_gather(rows_max, "c"), axis=0)
    rows_max = jnp.broadcast_to(rows_max[None], (ys * zls, *rows_max.shape))
    rows_max = jnp.max(all_to_all(rows_max, ("y", "zl")), axis=0)
    cols_max = jnp.broadcast_to(cols_max[None], (dp_count, *cols_max.shape))
    cols_max = jnp.max(all_to_all(cols_max, DP), axis=0)
    next_first_code = (
        first_new / (jnp.minimum(rows_max[0][:, None], cols_max[0][None, :]) + code_eps)
    ).astype(half)
    next_second_code = (
        second_new / (jnp.minimum(rows_max[1][:, None], cols_max[1][None, :]) + code_eps)
    ).astype(half)

    part = pl.pallas_call(
        cot_kernel,
        out_shape=(jax.ShapeDtypeStruct((zhs * seq, HD), half),) * xs,
        cost_estimate=pl.CostEstimate(flops=900000000, bytes_accessed=4000000, transcendentals=0),
    )(cot, weight_two, weight_far)
    part = exchanged(back(part), "x")
    part = summed(part).astype(half)
    part = exchanged(back([part[k * seq : (k + 1) * seq] for k in range(zhs)]), "zh")
    part = attend_back(probabilities, attended, summed(part).astype(half), key_sel, value_sel)
    heads = [part[k * quarter : (k + 1) * quarter] for k in range(zls)]
    came = swapped(jnp.stack([heads[2], heads[3]]), "zl", 2)
    last = swapped(jnp.stack([heads[1], came[1]]), "zl", 1)
    parts = jnp.stack([heads[0], came[0], last[0], last[1]])
    grad_queries = jnp.take(parts, inverse_of(zl_order), axis=0, mode="clip").reshape(seq, HD)
    return (
        grad_queries,
        new_weight,
        next_first_code,
        rows_max[0],
        cols_max[0],
        next_second_code,
        rows_max[1],
        cols_max[1],
    )


def inverse_of(order):
    return jnp.argmax(order[None, :] == jnp.arange(order.shape[0])[:, None], axis=1)


def solution(mesh):
    finer = Mesh(mesh.devices.reshape(4, 3, 8, 4, 2), (*DP, *TENSOR))
    placed = (
        P(DP, TENSOR),
        P(DP, None),
        P(DP, None),
        P(DP, TENSOR),
        P(DP, TENSOR),
        P(DP, TENSOR),
        P(DP),
        P(TENSOR),
        P(DP, TENSOR),
        P(DP),
        P(TENSOR),
    )
    return jax.shard_map(
        step,
        mesh=finer,
        in_specs=placed,
        out_specs=(
            P(DP, TENSOR),
            P(DP, TENSOR),
            P(DP, TENSOR),
            P(DP),
            P(TENSOR),
            P(DP, TENSOR),
            P(DP),
            P(TENSOR),
        ),
        check_vma=False,
    )
```

```python
import functools
import jax
import jax.numpy as jnp
from jax import lax
from jax.experimental import pallas as pl
from jax.experimental.pallas import tpu as pltpu
from jax.sharding import Mesh
from jax.sharding import PartitionSpec as P

H = 64
KVH = 8
HD = 128
DP = ("x", "zh")
TENSOR = ("y", "zl", "c")


beta_first = 0.9
beta_second = 0.95
learning = 0.01
decay_rate = 0.1
adam_eps = 1e-08
code_eps = 1e-06
correct_first = 1.0 - 0.9**10
correct_second = 1.0 - 0.95**10
half = jnp.bfloat16
full = jnp.float32
SPILL = 48


def shifted(block, axis, distance):
    size = lax.axis_size(axis)
    return lax.ppermute(block, axis, [(k, (k + distance) % size) for k in range(size)])


def swapped(block, axis, bit):
    size = lax.axis_size(axis)
    return lax.ppermute(block, axis, [(k, k ^ bit) for k in range(size)])


def summed(parts):
    total = parts[0].astype(full)
    for part in parts[1:]:
        total = total + part.astype(full)
    return total


def all_to_all(blocks, axes):
    return lax.all_to_all(blocks, axes, split_axis=0, concat_axis=0, tiled=True)


def attend(queries, key_sel, value_sel):
    shape = (queries.shape[0], key_sel.shape[0])
    scores = jnp.dot(queries, key_sel.T, preferred_element_type=full) * HD ** (-0.5)
    future = lax.broadcasted_iota(jnp.int32, shape, 1) > lax.broadcasted_iota(jnp.int32, shape, 0)
    scores = jnp.where(future, -1e30, scores)
    highest = jnp.max(scores, axis=-1, keepdims=True)
    exponent = jnp.exp(scores - highest)
    probabilities = exponent / jnp.sum(exponent, axis=-1, keepdims=True)
    attended = jnp.dot(probabilities.astype(half), value_sel, preferred_element_type=full)
    return probabilities, attended.astype(half)


def attend_back(probabilities, attended, grad_half, key_sel, value_sel):
    grad_probs = jnp.dot(grad_half, value_sel.T, preferred_element_type=full)
    row_dot = jnp.sum(grad_half.astype(full) * attended.astype(full), axis=-1, keepdims=True)
    grad_scores = (probabilities * (grad_probs - row_dot)).astype(half)
    return (jnp.dot(grad_scores, key_sel, preferred_element_type=full) * HD ** (-0.5)).astype(half)


def group_of(owner, zl, rows):
    return lax.shift_right_arithmetic(owner * rows - zl * (2 * HD) + 6 * HD, 10)


def weight_kernel(zhs, at_ref, weight_ref, own_ref, one_ref, two_ref, padded):
    rows = weight_ref.shape[0]
    owner, zl = at_ref[0] * zhs + at_ref[1], at_ref[2]
    pad = 2 * HD
    padded[...] = jnp.zeros_like(padded)
    padded[pad : pad + rows, :] = weight_ref[...]

    def put(bit, ref):
        place = zl ^ bit
        group = group_of(owner, place, rows)
        for k in range(2):
            start = group * 1024 + place * (2 * HD) + k * HD - owner * rows + pad
            inside = jnp.logical_and(start > pad - HD, start < pad + rows)
            start = pl.multiple_of(jnp.clip(start, 0, pad + rows), 16)
            block = padded[pl.ds(start, HD), :]
            ref[k * HD : (k + 1) * HD, :] = jnp.where(inside, block, 0.0).astype(half)

    put(0, own_ref)
    put(1, one_ref)
    put(2, two_ref.at[0])
    put(3, two_ref.at[1])


def weight_join_kernel(zhs, at_ref, *refs):
    parts, out_ref, scratch = refs[:-2], refs[-2], refs[-1]
    x, zh, zl = at_ref[0], at_ref[1], at_ref[2]
    rows = at_ref[4]
    scratch[...] = jnp.zeros_like(scratch)
    for back, part in enumerate(parts):
        at_zh = zh - back
        at_zh = jnp.where(at_zh < 0, at_zh + zhs, at_zh)
        group = jnp.clip(group_of(x * zhs + at_zh, zl, rows) - 2 * x, 0, 2)
        for h in range(4):
            scratch[group, h] = scratch[group, h] + part[h].astype(full)
    for h in range(4):
        for k in range(2):
            for c in range(2):
                start = (2 * c + k) * HD
                out_ref[h, start : start + HD, :] = scratch[k, h, c * HD : (c + 1) * HD, :].astype(half)
        out_ref[h, 4 * HD :, :] = scratch[2, h, :SPILL, :].astype(half)


def prepare_kernel(grad_ref, out_ref):
    turned = grad_ref[...].T
    for k in range(out_ref.shape[0]):
        out_ref[k] = turned


def out_kernel(at_ref, near_ref, far_ref, att_ref, came_ref, last_ref, out_ref, near_kept, far_kept, scratch, sems):
    core = at_ref[3]
    att = jnp.concatenate([att_ref[...], last_ref[0], came_ref[...], last_ref[1]], axis=1)
    places = out_ref.shape[0]
    scratch[places - 1, 4 * HD :, :] = jnp.zeros((SPILL, out_ref.shape[2]), half)
    copies = [
        pltpu.make_async_copy(near_ref, near_kept, sems.at[places]),
        pltpu.make_async_copy(far_ref, far_kept, sems.at[places + 1]),
    ]
    for copy in copies:
        copy.start()

    def put(part, c, k):
        whole = jnp.dot(part[2 * k : 2 * k + 2].reshape(2 * HD, -1), att, preferred_element_type=full)
        whole = whole.astype(half)
        for y in range(2):
            start = pl.multiple_of(y * 2 * HD + c * HD, HD)
            scratch[k, pl.ds(start, HD), :] = whole[y * HD : (y + 1) * HD]

    for k in range(places - 1, -1, -1):
        put(near_ref, core, k)
        put(far_ref, 1 - core, k)
        if k > 0:
            scratch[k - 1, 4 * HD :, :] = scratch[k, :SPILL, :]
        copy = pltpu.make_async_copy(scratch.at[k], out_ref.at[k], sems.at[k])
        copy.start()
        copies.append(copy)
    for copy in copies:
        copy.wait()


def send_kernel(zhs, at_ref, got_ref, out_ref, padded, sems):
    x, zl, rows = at_ref[0], at_ref[2], at_ref[4]
    sources, count = got_ref.shape[0], got_ref.shape[1]
    padded[count:, :] = jnp.zeros((padded.shape[0] - count, padded.shape[1]), half)

    def piece(r, carry):
        place = pl.ds(pl.multiple_of(r * 16, 16), 16)
        total = got_ref[0, place, :].astype(full)
        for d in range(1, sources):
            total = total + got_ref[d, place, :].astype(full)
        padded[place, :] = total.astype(half)
        return carry

    lax.fori_loop(0, count // 16, piece, 0, unroll=5)
    copies = []
    for z in range(zhs):
        group = jnp.clip(group_of(x * zhs + z, zl, rows) - 2 * x, 0, 2)
        start = pl.multiple_of(group * (2 * HD), 2 * HD)
        for h in range(4):
            block = padded.at[pl.ds(start, 2 * HD), h * HD : (h + 1) * HD]
            copy = pltpu.make_async_copy(block, out_ref.at[z * 4 + (zl ^ h)], sems.at[z * 4 + h])
            copy.start()
            copies.append(copy)
    for copy in copies:
        copy.wait()


def step_kernel(zhs, at_ref, got_ref, *refs):
    far_refs, (new_ref, first_new_ref, second_new_ref, rows_ref, cols_ref, held, padded, sizes, sems) = refs[:3], refs[3:]
    arrivals = [pltpu.make_async_copy(ref, held.at[k], sems.at[k]) for k, ref in enumerate(far_refs)]
    for copy in arrivals:
        copy.start()
    first_ref, second_ref, weight_ref = held.at[0], held.at[1], held.at[2]
    rows = weight_ref.shape[0]
    owner = at_ref[0] * zhs + at_ref[1]
    pad = HD
    padded[...] = jnp.zeros_like(padded)
    for place in range(4):
        total = got_ref[place].astype(full)
        for z in range(1, zhs):
            total = total + got_ref[z * 4 + place].astype(full)
        group = group_of(owner, place, rows)
        for k in range(2):
            start = group * 1024 + place * (2 * HD) + k * HD - owner * rows + pad
            inside = jnp.logical_and(jnp.logical_and(start > 0, start < pad + rows), group < 8)
            start = pl.multiple_of(jnp.where(inside, start, pad + rows), 16)
            padded[pl.ds(start, HD), :] = total[k * HD : (k + 1) * HD]

    per = 16
    for copy in arrivals:
        copy.wait()

    def piece(r, carry):
        place = pl.ds(pl.multiple_of(r * per, per), per)
        grad = padded[pl.ds(pl.multiple_of(r * per + pad, per), per), :]
        first_new = first_ref[place, :] + (1.0 - beta_first) * grad
        second_new = second_ref[place, :] + (1.0 - beta_second) * grad * grad
        size = first_new / correct_first / (jnp.sqrt(second_new / correct_second) + adam_eps)
        weight = weight_ref[place, :]
        new_ref[place, :] = weight - learning * (size + decay_rate * weight)
        first_new_ref[place, :] = first_new
        second_new_ref[place, :] = second_new
        first_abs, second_abs = jnp.abs(first_new), jnp.abs(second_new)
        sizes[0, place, :] = first_abs
        sizes[1, place, :] = second_abs
        return jnp.maximum(carry[0], first_abs), jnp.maximum(carry[1], second_abs)

    start = jnp.zeros((per, HD), full)
    most = lax.fori_loop(0, rows // per, piece, (start, start))
    for m in range(2):
        cols_ref[:, m, :] = jnp.broadcast_to(jnp.max(most[m], axis=0, keepdims=True), (cols_ref.shape[0], HD))
        for block in range(0, rows, HD):
            count = min(HD, rows - block)
            turned = jnp.max(sizes[m, block : block + HD, :].T, axis=0, keepdims=True)
            rows_ref[m : m + 1, block : block + count] = turned[:, :count]


def cot_kernel(at_ref, near_ref, far_ref, *refs):
    weights, out_refs = refs[:4], refs[4:]
    x, core = at_ref[0], at_ref[3]
    dims = (((0,), (0,)), ((), ()))
    groups, _, seq = near_ref.shape
    total = None
    extra_cot, extra_weight = [], []
    for back, weight in enumerate(weights):
        at_x = x - back
        at_x = jnp.where(at_x < 0, at_x + len(weights), at_x)
        wide = jnp.concatenate([weight[h] for h in range(4)], axis=1)
        for c in range(2):
            own, other = near_ref[pl.ds(2 * at_x, 2)], far_ref[pl.ds(2 * at_x, 2)]
            cot = jnp.where(core == c, own, other).reshape(2 * HD, seq)
            start = 2 * c * HD
            term = lax.dot_general(cot, wide[start : start + 2 * HD], dims, preferred_element_type=full)
            total = term if total is None else total + term
        y = jnp.minimum(2 * at_x + 2, groups - 1)
        extra_cot.append(jnp.where(core == 0, near_ref[y, :SPILL, :], far_ref[y, :SPILL, :]))
        extra_weight.append(wide[4 * HD :])
    extra_cot, extra_weight = jnp.concatenate(extra_cot, axis=0), jnp.concatenate(extra_weight, axis=0)
    total = total + lax.dot_general(extra_cot, extra_weight, dims, preferred_element_type=full)
    total = total.astype(half)
    out_refs[0][...] = total[:, :HD]
    out_refs[1][...] = total[:, HD : 2 * HD]
    out_refs[2][0] = total[:, 2 * HD : 3 * HD]
    out_refs[2][1] = total[:, 3 * HD :]


def step(
    queries,
    keys,
    values,
    grad_out,
    weight,
    first_code,
    first_rows,
    first_cols,
    second_code,
    second_rows,
    second_cols,
):
    dp_count = lax.axis_size(DP)
    ys, zls = lax.axis_size("y"), lax.axis_size("zl")
    xs, zhs = lax.axis_size("x"), lax.axis_size("zh")
    seq = queries.shape[0]
    rows = weight.shape[0]
    kv_start = lax.axis_index(TENSOR) // (H // KVH) * HD
    at = jnp.stack([lax.axis_index(axis) for axis in ("x", "zh", "zl", "c")] + [rows]).astype(jnp.int32)
    smem, vmem = pl.BlockSpec(memory_space=pltpu.SMEM), pl.BlockSpec(memory_space=pltpu.VMEM)
    shape = jax.ShapeDtypeStruct

    def kernel(body, arguments, outs, flops, room, scratch=(), space=vmem, spaces=None):
        return pl.pallas_call(
            body,
            out_shape=outs,
            in_specs=[smem] + (spaces or [vmem] * len(arguments)),
            out_specs=jax.tree.map(lambda _: space, outs),
            scratch_shapes=scratch,
            compiler_params=pltpu.CompilerParams(vmem_limit_bytes=room * 1024 * 1024),
            cost_estimate=pl.CostEstimate(flops=flops, bytes_accessed=3000000, transcendentals=0),
        )(at, *arguments)

    cot = pl.pallas_call(
        prepare_kernel,
        out_shape=shape((ys, HD, seq), half),
        compiler_params=pltpu.CompilerParams(vmem_limit_bytes=4 * 1024 * 1024),
    )(grad_out)
    near = all_to_all(cot, "y")
    far = shifted(near, "c", 1)

    own, one, two = kernel(
        functools.partial(weight_kernel, zhs),
        (weight,),
        (shape((2 * HD, HD), half), shape((2 * HD, HD), half), shape((2, 2 * HD, HD), half)),
        10000000,
        4,
        [pltpu.VMEM((rows + 4 * HD, HD), full)],
    )
    came = swapped(two, "zl", 2)
    last = swapped(jnp.stack([one, came[1]]), "zl", 1)
    part = jnp.stack([own, last[0], came[0], last[1]])

    key_sel = lax.dynamic_slice_in_dim(keys, kv_start, HD, 1)
    value_sel = lax.dynamic_slice_in_dim(values, kv_start, HD, 1)
    probabilities, attended = attend(queries, key_sel, value_sel)
    attended, probabilities = lax.optimization_barrier((attended, probabilities))
    came = swapped(attended, "zl", 2)
    last = swapped(jnp.stack([attended, came]), "zl", 1)

    hbm = pl.BlockSpec(memory_space=pltpu.HBM)
    in_hbm = functools.partial(pltpu.with_memory_space_constraint, memory_space=pltpu.HBM)
    cut = 4 * HD + SPILL
    kept = pltpu.HBM((ys, HD, seq), half)
    partial, near, far = kernel(
        out_kernel,
        (near, far, attended, came, last),
        (pltpu.HBM((xs, cut, zls * HD), half), kept, kept),
        800000000,
        16,
        [pltpu.VMEM((xs, cut, zls * HD), half), pltpu.SemaphoreType.DMA((xs + 2,))],
        hbm,
    )
    partial = all_to_all(partial, "x")
    partial = kernel(
        functools.partial(send_kernel, zhs),
        (partial,),
        pltpu.HBM((zhs * zls, 2 * HD, HD), half),
        10000000,
        10,
        [pltpu.VMEM((6 * HD, zls * HD), half), pltpu.SemaphoreType.DMA((zhs * zls,))],
        hbm,
    )
    partial = all_to_all(partial, ("zh", "zl"))
    first = beta_first * (first_code.astype(full) * jnp.minimum(first_rows[:, None], first_cols[None, :]))
    second = beta_second * (second_code.astype(full) * jnp.minimum(second_rows[:, None], second_cols[None, :]))
    moment = pltpu.HBM((rows, HD), full)
    new_weight, first_new, second_new, rows_max, cols_max = kernel(
        functools.partial(step_kernel, zhs),
        (partial, in_hbm(first), in_hbm(second), in_hbm(weight)),
        (moment, moment, moment, shape((2, rows), full), pltpu.HBM((dp_count, 2, HD), full)),
        10000000,
        8,
        [
            pltpu.VMEM((3, rows, HD), full),
            pltpu.VMEM((rows + 3 * HD, HD), full),
            pltpu.VMEM((2, -(-rows // HD) * HD, HD), full),
            pltpu.SemaphoreType.DMA((3,)),
        ],
        vmem,
        [vmem] + [hbm] * 3,
    )
    cols_max = jnp.max(all_to_all(cols_max, DP), axis=0)
    rows_max = jnp.max(lax.all_gather(rows_max, "c"), axis=0)
    rows_max = jnp.broadcast_to(rows_max[None], (ys * zls, *rows_max.shape))
    rows_max = jnp.max(all_to_all(rows_max, ("y", "zl")), axis=0)
    next_first_code = (
        first_new / (jnp.minimum(rows_max[0][:, None], cols_max[0][None, :]) + code_eps)
    ).astype(half)
    next_second_code = (
        second_new / (jnp.minimum(rows_max[1][:, None], cols_max[1][None, :]) + code_eps)
    ).astype(half)

    parts = [part] + [shifted(part, "zh", d) for d in range(1, zhs)]
    part = kernel(
        functools.partial(weight_join_kernel, zhs),
        parts,
        shape((zls, 4 * HD + SPILL, HD), half),
        10000000,
        6,
        [pltpu.VMEM((3, zls, 2 * HD, HD), full)],
    )
    before = shifted(part, "x", 1)
    after = shifted(part, "x", 3)
    parts = [part, before, shifted(before, "x", 1), after]
    own, one, two = kernel(
        cot_kernel,
        (near, far, *parts),
        (shape((seq, HD), half), shape((seq, HD), half), shape((2, seq, HD), half)),
        800000000,
        16,
    )
    came = swapped(two, "zl", 2)
    mid = summed([one, came[1]]).astype(half)
    last = swapped(mid, "zl", 1)
    grad_half = summed([own, came[0], last]).astype(half)
    grad_queries = attend_back(probabilities, attended, grad_half, key_sel, value_sel)
    return (
        grad_queries,
        new_weight,
        next_first_code,
        rows_max[0],
        cols_max[0],
        next_second_code,
        rows_max[1],
        cols_max[1],
    )


def solution(mesh):
    finer = Mesh(mesh.devices.reshape(4, 3, 8, 4, 2), (*DP, *TENSOR))
    placed = (
        P(DP, TENSOR),
        P(DP, None),
        P(DP, None),
        P(DP, TENSOR),
        P(DP, TENSOR),
        P(DP, TENSOR),
        P(DP),
        P(TENSOR),
        P(DP, TENSOR),
        P(DP),
        P(TENSOR),
    )
    return jax.shard_map(
        step,
        mesh=finer,
        in_specs=placed,
        out_specs=(
            P(DP, TENSOR),
            P(DP, TENSOR),
            P(DP, TENSOR),
            P(DP),
            P(TENSOR),
            P(DP, TENSOR),
            P(DP),
            P(TENSOR),
        ),
        check_vma=False,
    )
```

```python
import functools
import jax
import jax.numpy as jnp
from jax import lax
from jax.experimental import pallas as pl
from jax.experimental.pallas import tpu as pltpu
from jax.sharding import Mesh
from jax.sharding import PartitionSpec as P

H = 64
KVH = 8
HD = 128
DP = ("x", "zh")
TENSOR = ("y", "zl", "c")


beta_first = 0.9
beta_second = 0.95
learning = 0.01
decay_rate = 0.1
adam_eps = 1e-08
code_eps = 1e-06
correct_first = 1.0 - 0.9**10
correct_second = 1.0 - 0.95**10
half = jnp.bfloat16
full = jnp.float32
SPILL = 48


def shifted(block, axis, distance):
    size = lax.axis_size(axis)
    return lax.ppermute(block, axis, [(k, (k + distance) % size) for k in range(size)])


def swapped(block, axis, bit):
    size = lax.axis_size(axis)
    return lax.ppermute(block, axis, [(k, k ^ bit) for k in range(size)])


def summed(parts):
    total = parts[0].astype(full)
    for part in parts[1:]:
        total = total + part.astype(full)
    return total


def all_to_all(blocks, axes):
    return lax.all_to_all(blocks, axes, split_axis=0, concat_axis=0, tiled=True)


def attend(queries, key_sel, value_sel):
    shape = (queries.shape[0], key_sel.shape[0])
    scores = jnp.dot(queries, key_sel.T, preferred_element_type=full) * HD ** (-0.5)
    future = lax.broadcasted_iota(jnp.int32, shape, 1) > lax.broadcasted_iota(jnp.int32, shape, 0)
    scores = jnp.where(future, -1e30, scores)
    highest = jnp.max(scores, axis=-1, keepdims=True)
    exponent = jnp.exp(scores - highest)
    probabilities = exponent / jnp.sum(exponent, axis=-1, keepdims=True)
    attended = jnp.dot(probabilities.astype(half), value_sel, preferred_element_type=full)
    return probabilities, attended.astype(half)


def attend_back(probabilities, attended, grad_half, key_sel, value_sel):
    grad_probs = jnp.dot(grad_half, value_sel.T, preferred_element_type=full)
    row_dot = jnp.sum(grad_half.astype(full) * attended.astype(full), axis=-1, keepdims=True)
    grad_scores = (probabilities * (grad_probs - row_dot)).astype(half)
    return (jnp.dot(grad_scores, key_sel, preferred_element_type=full) * HD ** (-0.5)).astype(half)


def group_of(owner, zl, rows):
    return lax.shift_right_arithmetic(owner * rows - zl * (2 * HD) + 6 * HD, 10)


def weight_kernel(zhs, at_ref, weight_ref, own_ref, one_ref, two_ref, padded):
    rows = weight_ref.shape[0]
    owner, zl = at_ref[0] * zhs + at_ref[1], at_ref[2]
    pad = 2 * HD
    padded[...] = jnp.zeros_like(padded)
    padded[pad : pad + rows, :] = weight_ref[...]

    def put(bit, ref):
        place = zl ^ bit
        group = group_of(owner, place, rows)
        for k in range(2):
            start = group * 1024 + place * (2 * HD) + k * HD - owner * rows + pad
            inside = jnp.logical_and(start > pad - HD, start < pad + rows)
            start = pl.multiple_of(jnp.clip(start, 0, pad + rows), 16)
            block = padded[pl.ds(start, HD), :]
            ref[k * HD : (k + 1) * HD, :] = jnp.where(inside, block, 0.0).astype(half)

    put(0, own_ref)
    put(1, one_ref)
    put(2, two_ref.at[0])
    put(3, two_ref.at[1])


def weight_join_kernel(zhs, at_ref, *refs):
    parts, out_ref, scratch = refs[:-2], refs[-2], refs[-1]
    x, zh, zl = at_ref[0], at_ref[1], at_ref[2]
    rows = at_ref[4]
    scratch[...] = jnp.zeros_like(scratch)
    for back, part in enumerate(parts):
        at_zh = zh - back
        at_zh = jnp.where(at_zh < 0, at_zh + zhs, at_zh)
        group = jnp.clip(group_of(x * zhs + at_zh, zl, rows) - 2 * x, 0, 2)
        for h in range(4):
            scratch[group, h] = scratch[group, h] + part[h].astype(full)
    for h in range(4):
        for k in range(2):
            for c in range(2):
                start = (2 * c + k) * HD
                out_ref[h, start : start + HD, :] = scratch[k, h, c * HD : (c + 1) * HD, :].astype(half)
        out_ref[h, 4 * HD :, :] = scratch[2, h, :SPILL, :].astype(half)


def prepare_kernel(grad_ref, out_ref):
    turned = grad_ref[...].T
    for k in range(out_ref.shape[0]):
        out_ref[k] = turned


def out_kernel(at_ref, near_ref, far_ref, att_ref, came_ref, last_ref, out_ref, near_kept, far_kept, scratch, sems):
    core = at_ref[3]
    att = jnp.concatenate([att_ref[...], last_ref[0], came_ref[...], last_ref[1]], axis=1)
    places = out_ref.shape[0]
    scratch[places - 1, 4 * HD :, :] = jnp.zeros((SPILL, out_ref.shape[2]), half)
    copies = [
        pltpu.make_async_copy(near_ref, near_kept, sems.at[places]),
        pltpu.make_async_copy(far_ref, far_kept, sems.at[places + 1]),
    ]
    for copy in copies:
        copy.start()

    def put(part, c, k):
        whole = jnp.dot(part[2 * k : 2 * k + 2].reshape(2 * HD, -1), att, preferred_element_type=full)
        whole = whole.astype(half)
        for y in range(2):
            start = pl.multiple_of(y * 2 * HD + c * HD, HD)
            scratch[k, pl.ds(start, HD), :] = whole[y * HD : (y + 1) * HD]

    for k in range(places - 1, -1, -1):
        put(near_ref, core, k)
        put(far_ref, 1 - core, k)
        if k > 0:
            scratch[k - 1, 4 * HD :, :] = scratch[k, :SPILL, :]
        copy = pltpu.make_async_copy(scratch.at[k], out_ref.at[k], sems.at[k])
        copy.start()
        copies.append(copy)
    for copy in copies:
        copy.wait()


def send_kernel(zhs, at_ref, got_ref, out_ref, padded, sems):
    x, zl, rows = at_ref[0], at_ref[2], at_ref[4]
    sources, count = got_ref.shape[0], got_ref.shape[1]
    padded[count:, :] = jnp.zeros((padded.shape[0] - count, padded.shape[1]), half)

    def piece(r, carry):
        place = pl.ds(pl.multiple_of(r * 16, 16), 16)
        total = got_ref[0, place, :].astype(full)
        for d in range(1, sources):
            total = total + got_ref[d, place, :].astype(full)
        padded[place, :] = total.astype(half)
        return carry

    lax.fori_loop(0, count // 16, piece, 0, unroll=5)
    copies = []
    for z in range(zhs):
        group = jnp.clip(group_of(x * zhs + z, zl, rows) - 2 * x, 0, 2)
        start = pl.multiple_of(group * (2 * HD), 2 * HD)
        for h in range(4):
            block = padded.at[pl.ds(start, 2 * HD), h * HD : (h + 1) * HD]
            copy = pltpu.make_async_copy(block, out_ref.at[z * 4 + (zl ^ h)], sems.at[z * 4 + h])
            copy.start()
            copies.append(copy)
    for copy in copies:
        copy.wait()


def step_kernel(zhs, at_ref, got_ref, *refs):
    far_refs, (new_ref, first_new_ref, second_new_ref, rows_ref, cols_ref, held, padded, sizes, sems) = refs[:3], refs[3:]
    arrivals = [pltpu.make_async_copy(ref, held.at[k], sems.at[k]) for k, ref in enumerate(far_refs)]
    for copy in arrivals:
        copy.start()
    first_ref, second_ref, weight_ref = held.at[0], held.at[1], held.at[2]
    rows = weight_ref.shape[0]
    owner = at_ref[0] * zhs + at_ref[1]
    pad = HD
    padded[...] = jnp.zeros_like(padded)
    for place in range(4):
        total = got_ref[place].astype(full)
        for z in range(1, zhs):
            total = total + got_ref[z * 4 + place].astype(full)
        group = group_of(owner, place, rows)
        for k in range(2):
            start = group * 1024 + place * (2 * HD) + k * HD - owner * rows + pad
            inside = jnp.logical_and(jnp.logical_and(start > 0, start < pad + rows), group < 8)
            start = pl.multiple_of(jnp.where(inside, start, pad + rows), 16)
            padded[pl.ds(start, HD), :] = total[k * HD : (k + 1) * HD]

    per = 16
    for copy in arrivals:
        copy.wait()

    def piece(r, carry):
        place = pl.ds(pl.multiple_of(r * per, per), per)
        grad = padded[pl.ds(pl.multiple_of(r * per + pad, per), per), :]
        first_new = first_ref[place, :] + (1.0 - beta_first) * grad
        second_new = second_ref[place, :] + (1.0 - beta_second) * grad * grad
        size = first_new / correct_first / (jnp.sqrt(second_new / correct_second) + adam_eps)
        weight = weight_ref[place, :]
        new_ref[place, :] = weight - learning * (size + decay_rate * weight)
        first_new_ref[place, :] = first_new
        second_new_ref[place, :] = second_new
        first_abs, second_abs = jnp.abs(first_new), jnp.abs(second_new)
        sizes[0, place, :] = first_abs
        sizes[1, place, :] = second_abs
        return jnp.maximum(carry[0], first_abs), jnp.maximum(carry[1], second_abs)

    start = jnp.zeros((per, HD), full)
    most = lax.fori_loop(0, rows // per, piece, (start, start), unroll=True)
    for m in range(2):
        cols_ref[:, m, :] = jnp.broadcast_to(jnp.max(most[m], axis=0, keepdims=True), (cols_ref.shape[0], HD))
        for block in range(0, rows, HD):
            count = min(HD, rows - block)
            turned = jnp.max(sizes[m, block : block + HD, :].T, axis=0, keepdims=True)
            rows_ref[m : m + 1, block : block + count] = turned[:, :count]


def cot_terms(c_is_own, own, other, own_spill, other_spill, wide):
    dims = (((0,), (0,)), ((), ()))
    seq = own.shape[2]
    total = None
    for c in range(2):
        cot = jnp.where(c_is_own[c], own, other).reshape(2 * HD, seq)
        start = 2 * c * HD
        term = lax.dot_general(cot, wide[start : start + 2 * HD], dims, preferred_element_type=full)
        total = term if total is None else total + term
    cot = jnp.where(c_is_own[0], own_spill, other_spill)
    return total + lax.dot_general(cot, wide[4 * HD :], dims, preferred_element_type=full)


def placed_back(x, back, count):
    at_x = x - back
    return jnp.where(at_x < 0, at_x + count, at_x)


def cot_first_kernel(at_ref, near_ref, far_ref, *refs):
    weights, out_ref = refs[:3], refs[3]
    core = at_ref[3]
    groups = near_ref.shape[0]
    total = None
    for back, weight in zip((0, 1, 3), weights):
        at_x = placed_back(at_ref[0], back, groups // 2)
        wide = jnp.concatenate([weight[h] for h in range(4)], axis=1)
        y = jnp.minimum(2 * at_x + 2, groups - 1)
        pair = pl.ds(2 * at_x, 2)
        term = cot_terms(
            (core == 0, core == 1), near_ref[pair], far_ref[pair], near_ref[y, :SPILL], far_ref[y, :SPILL], wide
        )
        total = term if total is None else total + term
    out_ref[...] = total


def cot_last_kernel(at_ref, weight_ref, near_ref, far_ref, first_ref, *refs):
    own_ref, one_ref, two_ref, pairs, spills, first, sems = refs
    core = at_ref[3]
    groups = near_ref.shape[0]
    at_x = placed_back(at_ref[0], 2, groups // 2)
    y = jnp.minimum(2 * at_x + 2, groups - 1)
    copies = [pltpu.make_async_copy(first_ref, first, sems.at[4])]
    for k, ref in enumerate((near_ref, far_ref)):
        copies.append(pltpu.make_async_copy(ref.at[pl.ds(2 * at_x, 2)], pairs.at[k], sems.at[2 * k]))
        copies.append(pltpu.make_async_copy(ref.at[y, :SPILL], spills.at[k], sems.at[2 * k + 1]))
    for copy in copies:
        copy.start()
    wide = jnp.concatenate([weight_ref[h] for h in range(4)], axis=1)
    for copy in copies:
        copy.wait()
    total = cot_terms((core == 0, core == 1), pairs[0], pairs[1], spills[0], spills[1], wide)
    total = (first[...] + total).astype(half)
    own_ref[...] = total[:, :HD]
    one_ref[...] = total[:, HD : 2 * HD]
    two_ref[0] = total[:, 2 * HD : 3 * HD]
    two_ref[1] = total[:, 3 * HD :]


def step(
    queries,
    keys,
    values,
    grad_out,
    weight,
    first_code,
    first_rows,
    first_cols,
    second_code,
    second_rows,
    second_cols,
):
    dp_count = lax.axis_size(DP)
    ys, zls = lax.axis_size("y"), lax.axis_size("zl")
    xs, zhs = lax.axis_size("x"), lax.axis_size("zh")
    seq = queries.shape[0]
    rows = weight.shape[0]
    kv_start = lax.axis_index(TENSOR) // (H // KVH) * HD
    at = jnp.stack([lax.axis_index(axis) for axis in ("x", "zh", "zl", "c")] + [rows]).astype(jnp.int32)
    smem, vmem = pl.BlockSpec(memory_space=pltpu.SMEM), pl.BlockSpec(memory_space=pltpu.VMEM)
    shape = jax.ShapeDtypeStruct

    def kernel(body, arguments, outs, flops, room, scratch=(), space=vmem, spaces=None):
        return pl.pallas_call(
            body,
            out_shape=outs,
            in_specs=[smem] + (spaces or [vmem] * len(arguments)),
            out_specs=jax.tree.map(lambda _: space, outs),
            scratch_shapes=scratch,
            compiler_params=pltpu.CompilerParams(vmem_limit_bytes=room * 1024 * 1024),
            cost_estimate=pl.CostEstimate(flops=flops, bytes_accessed=3000000, transcendentals=0),
        )(at, *arguments)

    cot = pl.pallas_call(
        prepare_kernel,
        out_shape=shape((ys, HD, seq), half),
        compiler_params=pltpu.CompilerParams(vmem_limit_bytes=4 * 1024 * 1024),
    )(grad_out)
    near = all_to_all(cot, "y")
    far = shifted(near, "c", 1)

    own, one, two = kernel(
        functools.partial(weight_kernel, zhs),
        (weight,),
        (shape((2 * HD, HD), half), shape((2 * HD, HD), half), shape((2, 2 * HD, HD), half)),
        10000000,
        4,
        [pltpu.VMEM((rows + 4 * HD, HD), full)],
    )
    came = swapped(two, "zl", 2)
    last = swapped(jnp.stack([one, came[1]]), "zl", 1)
    part = jnp.stack([own, last[0], came[0], last[1]])

    key_sel = lax.dynamic_slice_in_dim(keys, kv_start, HD, 1)
    value_sel = lax.dynamic_slice_in_dim(values, kv_start, HD, 1)
    probabilities, attended = attend(queries, key_sel, value_sel)
    attended, probabilities = lax.optimization_barrier((attended, probabilities))
    came = swapped(attended, "zl", 2)
    last = swapped(jnp.stack([attended, came]), "zl", 1)

    hbm = pl.BlockSpec(memory_space=pltpu.HBM)
    in_hbm = functools.partial(pltpu.with_memory_space_constraint, memory_space=pltpu.HBM)
    cut = 4 * HD + SPILL
    kept = pltpu.HBM((ys, HD, seq), half)
    partial, near, far = kernel(
        out_kernel,
        (near, far, attended, came, last),
        (pltpu.HBM((xs, cut, zls * HD), half), kept, kept),
        800000000,
        16,
        [pltpu.VMEM((xs, cut, zls * HD), half), pltpu.SemaphoreType.DMA((xs + 2,))],
        hbm,
    )
    partial = all_to_all(partial, "x")
    partial = kernel(
        functools.partial(send_kernel, zhs),
        (partial,),
        pltpu.HBM((zhs * zls, 2 * HD, HD), half),
        10000000,
        10,
        [pltpu.VMEM((6 * HD, zls * HD), half), pltpu.SemaphoreType.DMA((zhs * zls,))],
        hbm,
    )
    partial = all_to_all(partial, ("zh", "zl"))
    first = beta_first * (first_code.astype(full) * jnp.minimum(first_rows[:, None], first_cols[None, :]))
    second = beta_second * (second_code.astype(full) * jnp.minimum(second_rows[:, None], second_cols[None, :]))
    moment = pltpu.HBM((rows, HD), full)
    new_weight, first_new, second_new, rows_max, cols_max = kernel(
        functools.partial(step_kernel, zhs),
        (partial, in_hbm(first), in_hbm(second), in_hbm(weight)),
        (moment, moment, moment, shape((2, rows), full), pltpu.HBM((dp_count, 2, HD), full)),
        10000000,
        8,
        [
            pltpu.VMEM((3, rows, HD), full),
            pltpu.VMEM((rows + 3 * HD, HD), full),
            pltpu.VMEM((2, -(-rows // HD) * HD, HD), full),
            pltpu.SemaphoreType.DMA((3,)),
        ],
        vmem,
        [vmem] + [hbm] * 3,
    )
    cols_max = jnp.max(all_to_all(cols_max, DP), axis=0)
    rows_max = jnp.max(lax.all_gather(rows_max, "c"), axis=0)
    rows_max = jnp.broadcast_to(rows_max[None], (ys * zls, *rows_max.shape))
    rows_max = jnp.max(all_to_all(rows_max, ("y", "zl")), axis=0)
    next_first_code = (
        first_new / (jnp.minimum(rows_max[0][:, None], cols_max[0][None, :]) + code_eps)
    ).astype(half)
    next_second_code = (
        second_new / (jnp.minimum(rows_max[1][:, None], cols_max[1][None, :]) + code_eps)
    ).astype(half)

    parts = [part] + [shifted(part, "zh", d) for d in range(1, zhs)]
    part = kernel(
        functools.partial(weight_join_kernel, zhs),
        parts,
        shape((zls, 4 * HD + SPILL, HD), half),
        10000000,
        6,
        [pltpu.VMEM((3, zls, 2 * HD, HD), full)],
    )
    before = shifted(part, "x", 1)
    after = shifted(part, "x", 3)
    beyond = shifted(before, "x", 1)
    cot = kernel(cot_first_kernel, (near, far, part, before, after), pltpu.HBM((seq, zls * HD), full), 600000000, 16)
    own, one, two = kernel(
        cot_last_kernel,
        (beyond, in_hbm(near), in_hbm(far), in_hbm(cot)),
        (shape((seq, HD), half), shape((seq, HD), half), shape((2, seq, HD), half)),
        200000000,
        12,
        [
            pltpu.VMEM((2, 2, HD, seq), half),
            pltpu.VMEM((2, SPILL, seq), half),
            pltpu.VMEM((seq, zls * HD), full),
            pltpu.SemaphoreType.DMA((5,)),
        ],
        vmem,
        [vmem] + [hbm] * 3,
    )
    came = swapped(two, "zl", 2)
    mid = summed([one, came[1]]).astype(half)
    last = swapped(mid, "zl", 1)
    grad_half = summed([own, came[0], last]).astype(half)
    grad_queries = attend_back(probabilities, attended, grad_half, key_sel, value_sel)
    return (
        grad_queries,
        new_weight,
        next_first_code,
        rows_max[0],
        cols_max[0],
        next_second_code,
        rows_max[1],
        cols_max[1],
    )


def solution(mesh):
    finer = Mesh(mesh.devices.reshape(4, 3, 8, 4, 2), (*DP, *TENSOR))
    placed = (
        P(DP, TENSOR),
        P(DP, None),
        P(DP, None),
        P(DP, TENSOR),
        P(DP, TENSOR),
        P(DP, TENSOR),
        P(DP),
        P(TENSOR),
        P(DP, TENSOR),
        P(DP),
        P(TENSOR),
    )
    return jax.shard_map(
        step,
        mesh=finer,
        in_specs=placed,
        out_specs=(
            P(DP, TENSOR),
            P(DP, TENSOR),
            P(DP, TENSOR),
            P(DP),
            P(TENSOR),
            P(DP, TENSOR),
            P(DP),
            P(TENSOR),
        ),
        check_vma=False,
    )
```

```python
import functools
import jax
import jax.numpy as jnp
from jax import lax
from jax.experimental import pallas as pl
from jax.experimental.pallas import tpu as pltpu
from jax.sharding import Mesh
from jax.sharding import PartitionSpec as P

H = 64
KVH = 8
HD = 128
DP = ("x", "zh")
TENSOR = ("y", "zl", "c")


beta_first = 0.9
beta_second = 0.95
learning = 0.01
decay_rate = 0.1
adam_eps = 1e-08
code_eps = 1e-06
correct_first = 1.0 - 0.9**10
correct_second = 1.0 - 0.95**10
half = jnp.bfloat16
full = jnp.float32
SPILL = 48
EXTRA = 16


def shifted(block, axis, distance):
    size = lax.axis_size(axis)
    return lax.ppermute(block, axis, [(k, (k + distance) % size) for k in range(size)])


def swapped(block, axis, bit):
    size = lax.axis_size(axis)
    return lax.ppermute(block, axis, [(k, k ^ bit) for k in range(size)])


def summed(parts):
    total = parts[0].astype(full)
    for part in parts[1:]:
        total = total + part.astype(full)
    return total


def all_to_all(blocks, axes):
    return lax.all_to_all(blocks, axes, split_axis=0, concat_axis=0, tiled=True)


def attend(queries, key_sel, value_sel):
    shape = (queries.shape[0], key_sel.shape[0])
    scores = jnp.dot(queries, key_sel.T, preferred_element_type=full) * HD ** (-0.5)
    future = lax.broadcasted_iota(jnp.int32, shape, 1) > lax.broadcasted_iota(jnp.int32, shape, 0)
    scores = jnp.where(future, -1e30, scores)
    highest = jnp.max(scores, axis=-1, keepdims=True)
    exponent = jnp.exp(scores - highest)
    probabilities = exponent / jnp.sum(exponent, axis=-1, keepdims=True)
    attended = jnp.dot(probabilities.astype(half), value_sel, preferred_element_type=full)
    return probabilities, attended.astype(half)


def attend_back(probabilities, attended, grad_half, key_sel, value_sel):
    grad_probs = jnp.dot(grad_half, value_sel.T, preferred_element_type=full)
    row_dot = jnp.sum(grad_half.astype(full) * attended.astype(full), axis=-1, keepdims=True)
    grad_scores = (probabilities * (grad_probs - row_dot)).astype(half)
    return (jnp.dot(grad_scores, key_sel, preferred_element_type=full) * HD ** (-0.5)).astype(half)


def group_of(owner, zl, rows):
    return lax.shift_right_arithmetic(owner * rows - zl * (2 * HD) + 6 * HD, 10)


def weight_kernel(zhs, at_ref, weight_ref, own_ref, one_ref, two_ref, padded):
    rows = weight_ref.shape[0]
    owner, zl = at_ref[0] * zhs + at_ref[1], at_ref[2]
    pad = 2 * HD
    padded[...] = jnp.zeros_like(padded)
    padded[pad : pad + rows, :] = weight_ref[...]

    def put(bit, ref):
        place = zl ^ bit
        group = group_of(owner, place, rows)
        for k in range(2):
            start = group * 1024 + place * (2 * HD) + k * HD - owner * rows + pad
            inside = jnp.logical_and(start > pad - HD, start < pad + rows)
            start = pl.multiple_of(jnp.clip(start, 0, pad + rows), 16)
            block = padded[pl.ds(start, HD), :]
            ref[k * HD : (k + 1) * HD, :] = jnp.where(inside, block, 0.0).astype(half)

    put(0, own_ref)
    put(1, one_ref)
    put(2, two_ref.at[0])
    put(3, two_ref.at[1])


def weight_join_kernel(zhs, at_ref, *refs):
    parts, out_ref, scratch = refs[:-2], refs[-2], refs[-1]
    x, zh, zl = at_ref[0], at_ref[1], at_ref[2]
    rows = at_ref[4]
    scratch[...] = jnp.zeros_like(scratch)
    for back, part in enumerate(parts):
        at_zh = zh - back
        at_zh = jnp.where(at_zh < 0, at_zh + zhs, at_zh)
        group = jnp.clip(group_of(x * zhs + at_zh, zl, rows) - 2 * x, 0, 2)
        for h in range(4):
            scratch[group, h] = scratch[group, h] + part[h].astype(full)
    for h in range(4):
        for k in range(2):
            for c in range(2):
                start = (2 * c + k) * HD
                out_ref[h, start : start + HD, :] = scratch[k, h, c * HD : (c + 1) * HD, :].astype(half)
        out_ref[h, 4 * HD :, :] = scratch[2, h, :SPILL, :].astype(half)


def prepare_kernel(grad_ref, out_ref):
    turned = grad_ref[...].T
    for k in range(out_ref.shape[0]):
        out_ref[k] = turned


def out_kernel(side, at_ref, part_ref, att_ref, came_ref, last_ref, *refs):
    out_ref, kept_ref, scratch, firsts, sems = refs[-5:]
    zl, core = at_ref[2], at_ref[3]
    c = core if side == 0 else 1 - core
    spilling = jnp.logical_and(zl == 0, c == 0)
    att = jnp.concatenate([att_ref[...], last_ref[0], came_ref[...], last_ref[1]], axis=1)
    groups = part_ref.shape[0]
    places = groups // 2
    copies = [pltpu.make_async_copy(part_ref, kept_ref, sems.at[groups])]
    if side == 1:
        scratch[groups, :EXTRA, :] = jnp.zeros((EXTRA, out_ref.shape[2]), half)
        copies.append(
            pltpu.make_async_copy(
                scratch.at[groups, :EXTRA], out_ref.at[places - 1, 4 * HD :], sems.at[groups + places]
            )
        )
    for copy in copies:
        copy.start()
    for k in range(places - 1, -1, -1):
        whole = jnp.dot(part_ref[2 * k : 2 * k + 2].reshape(2 * HD, -1), att, preferred_element_type=full).astype(half)
        scratch[2 * k : 2 * k + 2] = whole.reshape(2, HD, -1)
        firsts[k] = whole[:SPILL]
        if 0 < k < places - 1:
            rows = k * EXTRA
            scratch[2 * k, :rows, :] = jnp.where(spilling, firsts[k + 1, :rows, :], whole[:rows])
        for y in range(2):
            start = pl.multiple_of(y * 2 * HD + c * HD, HD)
            copy = pltpu.make_async_copy(scratch.at[2 * k + y], out_ref.at[k, pl.ds(start, HD)], sems.at[2 * k + y])
            copy.start()
            copies.append(copy)

    @pl.when(c == 0)
    def _():
        spills = [
            pltpu.make_async_copy(
                firsts.at[k + 1, k * EXTRA : (k + 1) * EXTRA], out_ref.at[k, 4 * HD :], sems.at[groups + 1 + k]
            )
            for k in range(places - 1)
        ]
        for copy in spills:
            copy.start()
        for copy in spills:
            copy.wait()

    for copy in copies:
        copy.wait()


def send_kernel(zhs, at_ref, got_ref, out_ref, padded, sems):
    x, zl, rows = at_ref[0], at_ref[2], at_ref[4]
    sources, count = got_ref.shape[0], got_ref.shape[1] - EXTRA
    padded[count:, :] = jnp.zeros((padded.shape[0] - count, padded.shape[1]), half)

    def summed_at(place):
        total = got_ref[0, place, :].astype(full)
        for d in range(1, sources):
            total = total + got_ref[d, place, :].astype(full)
        return total.astype(half)

    def piece(r, carry):
        place = pl.ds(pl.multiple_of(r * 16, 16), 16)
        padded[place, :] = summed_at(place)
        return carry

    lax.fori_loop(0, count // 16, piece, 0, unroll=4)
    padded[count : count + SPILL, :] = padded[:SPILL, :]
    last = pl.ds(pl.multiple_of(count + x * EXTRA, EXTRA), EXTRA)
    padded[last, :] = summed_at(slice(count, count + EXTRA))
    copies = []
    for z in range(zhs):
        group = jnp.clip(group_of(x * zhs + z, zl, rows) - 2 * x, 0, 2)
        start = pl.multiple_of(group * (2 * HD), 2 * HD)
        for h in range(4):
            block = padded.at[pl.ds(start, 2 * HD), h * HD : (h + 1) * HD]
            copy = pltpu.make_async_copy(block, out_ref.at[z * 4 + (zl ^ h)], sems.at[z * 4 + h])
            copy.start()
            copies.append(copy)
    for copy in copies:
        copy.wait()


def step_kernel(zhs, at_ref, got_ref, *refs):
    far_refs, (new_ref, first_new_ref, second_new_ref, rows_ref, cols_ref, held, padded, sizes, sems) = refs[:3], refs[3:]
    arrivals = [pltpu.make_async_copy(ref, held.at[k], sems.at[k]) for k, ref in enumerate(far_refs)]
    for copy in arrivals:
        copy.start()
    first_ref, second_ref, weight_ref = held.at[0], held.at[1], held.at[2]
    rows = weight_ref.shape[0]
    owner = at_ref[0] * zhs + at_ref[1]
    pad = HD
    padded[...] = jnp.zeros_like(padded)
    for place in range(4):
        total = got_ref[place].astype(full)
        for z in range(1, zhs):
            total = total + got_ref[z * 4 + place].astype(full)
        group = group_of(owner, place, rows)
        for k in range(2):
            start = group * 1024 + place * (2 * HD) + k * HD - owner * rows + pad
            inside = jnp.logical_and(jnp.logical_and(start > 0, start < pad + rows), group < 8)
            start = pl.multiple_of(jnp.where(inside, start, pad + rows), 16)
            padded[pl.ds(start, HD), :] = total[k * HD : (k + 1) * HD]

    per = 16
    for copy in arrivals:
        copy.wait()

    def piece(r, carry):
        place = pl.ds(pl.multiple_of(r * per, per), per)
        grad = padded[pl.ds(pl.multiple_of(r * per + pad, per), per), :]
        first_new = first_ref[place, :] + (1.0 - beta_first) * grad
        second_new = second_ref[place, :] + (1.0 - beta_second) * grad * grad
        size = first_new / correct_first / (jnp.sqrt(second_new / correct_second) + adam_eps)
        weight = weight_ref[place, :]
        new_ref[place, :] = weight - learning * (size + decay_rate * weight)
        first_new_ref[place, :] = first_new
        second_new_ref[place, :] = second_new
        first_abs, second_abs = jnp.abs(first_new), jnp.abs(second_new)
        sizes[0, place, :] = first_abs
        sizes[1, place, :] = second_abs
        return jnp.maximum(carry[0], first_abs), jnp.maximum(carry[1], second_abs)

    start = jnp.zeros((per, HD), full)
    most = lax.fori_loop(0, rows // per, piece, (start, start), unroll=True)
    for m in range(2):
        cols_ref[:, m, :] = jnp.broadcast_to(jnp.max(most[m], axis=0, keepdims=True), (cols_ref.shape[0], HD))
        for block in range(0, rows, HD):
            count = min(HD, rows - block)
            turned = jnp.max(sizes[m, block : block + HD, :].T, axis=0, keepdims=True)
            rows_ref[m : m + 1, block : block + count] = turned[:, :count]


def cot_terms(c_is_own, own, other, own_spill, other_spill, wide):
    dims = (((0,), (0,)), ((), ()))
    seq = own.shape[2]
    total = None
    for c in range(2):
        cot = jnp.where(c_is_own[c], own, other).reshape(2 * HD, seq)
        start = 2 * c * HD
        term = lax.dot_general(cot, wide[start : start + 2 * HD], dims, preferred_element_type=full)
        total = term if total is None else total + term
    cot = jnp.where(c_is_own[0], own_spill, other_spill)
    return total + lax.dot_general(cot, wide[4 * HD :], dims, preferred_element_type=full)


def placed_back(x, back, count):
    at_x = x - back
    return jnp.where(at_x < 0, at_x + count, at_x)


def cot_first_kernel(at_ref, near_ref, far_ref, *refs):
    weights, out_ref = refs[:3], refs[3]
    core = at_ref[3]
    groups = near_ref.shape[0]
    total = None
    for back, weight in zip((0, 1, 3), weights):
        at_x = placed_back(at_ref[0], back, groups // 2)
        wide = jnp.concatenate([weight[h] for h in range(4)], axis=1)
        y = jnp.minimum(2 * at_x + 2, groups - 1)
        pair = pl.ds(2 * at_x, 2)
        term = cot_terms(
            (core == 0, core == 1), near_ref[pair], far_ref[pair], near_ref[y, :SPILL], far_ref[y, :SPILL], wide
        )
        total = term if total is None else total + term
    out_ref[...] = total


def cot_last_kernel(at_ref, weight_ref, near_ref, far_ref, first_ref, *refs):
    own_ref, one_ref, two_ref, pairs, spills, first, sems = refs
    core = at_ref[3]
    groups = near_ref.shape[0]
    at_x = placed_back(at_ref[0], 2, groups // 2)
    y = jnp.minimum(2 * at_x + 2, groups - 1)
    copies = [pltpu.make_async_copy(first_ref, first, sems.at[4])]
    for k, ref in enumerate((near_ref, far_ref)):
        copies.append(pltpu.make_async_copy(ref.at[pl.ds(2 * at_x, 2)], pairs.at[k], sems.at[2 * k]))
        copies.append(pltpu.make_async_copy(ref.at[y, :SPILL], spills.at[k], sems.at[2 * k + 1]))
    for copy in copies:
        copy.start()
    wide = jnp.concatenate([weight_ref[h] for h in range(4)], axis=1)
    for copy in copies:
        copy.wait()
    total = cot_terms((core == 0, core == 1), pairs[0], pairs[1], spills[0], spills[1], wide)
    total = (first[...] + total).astype(half)
    own_ref[...] = total[:, :HD]
    one_ref[...] = total[:, HD : 2 * HD]
    two_ref[0] = total[:, 2 * HD : 3 * HD]
    two_ref[1] = total[:, 3 * HD :]


def step(
    queries,
    keys,
    values,
    grad_out,
    weight,
    first_code,
    first_rows,
    first_cols,
    second_code,
    second_rows,
    second_cols,
):
    dp_count = lax.axis_size(DP)
    ys, zls = lax.axis_size("y"), lax.axis_size("zl")
    xs, zhs = lax.axis_size("x"), lax.axis_size("zh")
    seq = queries.shape[0]
    rows = weight.shape[0]
    kv_start = lax.axis_index(TENSOR) // (H // KVH) * HD
    at = jnp.stack([lax.axis_index(axis) for axis in ("x", "zh", "zl", "c")] + [rows]).astype(jnp.int32)
    smem, vmem = pl.BlockSpec(memory_space=pltpu.SMEM), pl.BlockSpec(memory_space=pltpu.VMEM)
    shape = jax.ShapeDtypeStruct

    def kernel(body, arguments, outs, flops, room, scratch=(), space=vmem, spaces=None, aliases={}):
        return pl.pallas_call(
            body,
            out_shape=outs,
            in_specs=[smem] + (spaces or [vmem] * len(arguments)),
            out_specs=jax.tree.map(lambda _: space, outs),
            scratch_shapes=scratch,
            input_output_aliases=aliases,
            compiler_params=pltpu.CompilerParams(vmem_limit_bytes=room * 1024 * 1024),
            cost_estimate=pl.CostEstimate(flops=flops, bytes_accessed=3000000, transcendentals=0),
        )(at, *arguments)

    cot = pl.pallas_call(
        prepare_kernel,
        out_shape=shape((ys, HD, seq), half),
        compiler_params=pltpu.CompilerParams(vmem_limit_bytes=4 * 1024 * 1024),
    )(grad_out)
    near = all_to_all(cot, "y")
    far = shifted(near, "c", 1)

    own, one, two = kernel(
        functools.partial(weight_kernel, zhs),
        (weight,),
        (shape((2 * HD, HD), half), shape((2 * HD, HD), half), shape((2, 2 * HD, HD), half)),
        10000000,
        4,
        [pltpu.VMEM((rows + 4 * HD, HD), full)],
    )
    came = swapped(two, "zl", 2)
    last = swapped(jnp.stack([one, came[1]]), "zl", 1)
    part = jnp.stack([own, last[0], came[0], last[1]])

    key_sel = lax.dynamic_slice_in_dim(keys, kv_start, HD, 1)
    value_sel = lax.dynamic_slice_in_dim(values, kv_start, HD, 1)
    probabilities, attended = attend(queries, key_sel, value_sel)
    attended, probabilities = lax.optimization_barrier((attended, probabilities))
    came = swapped(attended, "zl", 2)
    last = swapped(jnp.stack([attended, came]), "zl", 1)

    hbm = pl.BlockSpec(memory_space=pltpu.HBM)
    in_hbm = functools.partial(pltpu.with_memory_space_constraint, memory_space=pltpu.HBM)
    cut = 4 * HD + EXTRA
    kept = pltpu.HBM((ys, HD, seq), half)
    made = pltpu.HBM((xs, cut, zls * HD), half)
    room = [
        pltpu.VMEM((ys + 1, HD, zls * HD), half),
        pltpu.VMEM((xs, SPILL, zls * HD), half),
        pltpu.SemaphoreType.DMA((ys + 1 + xs,)),
    ]
    att = (attended, came, last)
    partial, near = kernel(functools.partial(out_kernel, 0), (near, *att), (made, kept), 400000000, 12, room, hbm)
    partial, far = kernel(
        functools.partial(out_kernel, 1),
        (far, *att, partial),
        (made, kept),
        400000000,
        12,
        room,
        hbm,
        [vmem] * 4 + [hbm],
        {5: 0},
    )
    partial = all_to_all(partial, "x")
    partial = kernel(
        functools.partial(send_kernel, zhs),
        (partial,),
        pltpu.HBM((zhs * zls, 2 * HD, HD), half),
        10000000,
        10,
        [pltpu.VMEM((6 * HD, zls * HD), half), pltpu.SemaphoreType.DMA((zhs * zls,))],
        hbm,
    )
    partial = all_to_all(partial, ("zh", "zl"))
    first = beta_first * (first_code.astype(full) * jnp.minimum(first_rows[:, None], first_cols[None, :]))
    second = beta_second * (second_code.astype(full) * jnp.minimum(second_rows[:, None], second_cols[None, :]))
    moment = pltpu.HBM((rows, HD), full)
    new_weight, first_new, second_new, rows_max, cols_max = kernel(
        functools.partial(step_kernel, zhs),
        (partial, in_hbm(first), in_hbm(second), in_hbm(weight)),
        (moment, moment, moment, shape((2, rows), full), pltpu.HBM((dp_count, 2, HD), full)),
        10000000,
        8,
        [
            pltpu.VMEM((3, rows, HD), full),
            pltpu.VMEM((rows + 3 * HD, HD), full),
            pltpu.VMEM((2, -(-rows // HD) * HD, HD), full),
            pltpu.SemaphoreType.DMA((3,)),
        ],
        vmem,
        [vmem] + [hbm] * 3,
    )
    cols_max = jnp.max(all_to_all(cols_max, DP), axis=0)
    rows_max = jnp.max(lax.all_gather(rows_max, "c"), axis=0)
    rows_max = jnp.broadcast_to(rows_max.astype(half)[None], (ys * zls, *rows_max.shape))
    rows_max = all_to_all(rows_max, ("y", "zl"))
    rows_max = jnp.max(rows_max.astype(full), axis=0)
    next_first_code = (first_new / (jnp.minimum(rows_max[0][:, None], cols_max[0][None, :]) + code_eps)).astype(half)
    next_second_code = (second_new / (jnp.minimum(rows_max[1][:, None], cols_max[1][None, :]) + code_eps)).astype(half)

    parts = [part] + [shifted(part, "zh", d) for d in range(1, zhs)]
    part = kernel(
        functools.partial(weight_join_kernel, zhs),
        parts,
        shape((zls, 4 * HD + SPILL, HD), half),
        10000000,
        6,
        [pltpu.VMEM((3, zls, 2 * HD, HD), full)],
    )
    before = shifted(part, "x", 1)
    after = shifted(part, "x", 3)
    beyond = shifted(before, "x", 1)
    cot = kernel(cot_first_kernel, (near, far, part, before, after), pltpu.HBM((seq, zls * HD), full), 600000000, 16)
    own, one, two = kernel(
        cot_last_kernel,
        (beyond, in_hbm(near), in_hbm(far), in_hbm(cot)),
        (shape((seq, HD), half), shape((seq, HD), half), shape((2, seq, HD), half)),
        200000000,
        12,
        [
            pltpu.VMEM((2, 2, HD, seq), half),
            pltpu.VMEM((2, SPILL, seq), half),
            pltpu.VMEM((seq, zls * HD), full),
            pltpu.SemaphoreType.DMA((5,)),
        ],
        vmem,
        [vmem] + [hbm] * 3,
    )
    came = swapped(two, "zl", 2)
    mid = summed([one, came[1]]).astype(half)
    last = swapped(mid, "zl", 1)
    grad_half = summed([own, came[0], last]).astype(half)
    grad_queries = attend_back(probabilities, attended, grad_half, key_sel, value_sel)
    return (
        grad_queries,
        new_weight,
        next_first_code,
        rows_max[0],
        cols_max[0],
        next_second_code,
        rows_max[1],
        cols_max[1],
    )


def solution(mesh):
    finer = Mesh(mesh.devices.reshape(4, 3, 8, 4, 2), (*DP, *TENSOR))
    placed = (
        P(DP, TENSOR),
        P(DP, None),
        P(DP, None),
        P(DP, TENSOR),
        P(DP, TENSOR),
        P(DP, TENSOR),
        P(DP),
        P(TENSOR),
        P(DP, TENSOR),
        P(DP),
        P(TENSOR),
    )
    return jax.shard_map(
        step,
        mesh=finer,
        in_specs=placed,
        out_specs=(
            P(DP, TENSOR),
            P(DP, TENSOR),
            P(DP, TENSOR),
            P(DP),
            P(TENSOR),
            P(DP, TENSOR),
            P(DP),
            P(TENSOR),
        ),
        check_vma=False,
    )
```
